32 devices in a mesh: chan: 16 (over z, y, x), tm: 2 (over core).
Axes of the slice: x: 2, y: 2, z: 4, core: 2. Of those that a mesh axis runs over, the one named last changes fastest.
Arguments:
- visibilities: bfloat16 [2, 4, 128, 480], P(None, 'tm', 'chan'), may hold values from -6 to 6
- baseline_coords: float32 [3, 4, 480], P(None, 'tm'), may hold values from -180 to 180
- source_offsets: float32 [2, 20], replicated, may hold values from -0.08 to 0.08
- source_flux: float32 [20, 128], P(None, 'chan'), may hold values from 0.01 to 0.1
- cluster_of_source: int32 [20, 1], replicated, may hold values from 0 to 17
- baseline_stations: int32 [480, 2], replicated, may hold values from 0 to 61, as said below
- station_flags: int32 [62, 4], P(None, 'tm'), may hold values 0 or 1
- local_gains: float32 [2, 2, 128, 18, 62], P(None, 'tm', 'chan'), may hold values from -1.6 to 3.2
- dual_gains: float32 [2, 2, 128, 18, 62], P(None, 'tm', 'chan'), may hold values from -3.5 to 3.5
- penalty: float32 [18], replicated, may hold values from 0.4 to 0.8
Outputs:
- cross_power: float32 [480, 128], P('chan', 'tm')
- dual_update: float32 [2, 2, 128, 18, 62], P(None, 'tm', 'chan')
The draws below stay inside these ranges and needn't reach their ends.
Inputs may be any that keep to these rules, and one draw needn't show every extreme that they name: `baseline_stations`: row b holds two different stations, the first the smaller; rows repeat a pair only where 480 exceeds the number of station pairs. `cluster_of_source`: every direction has at least one component.
All inputs are finite; a program needn't handle non-finite values. No bound on the sum of `station_flags` on one device may be relied on, other than what follows from the above.
Results may differ from the reference program's by a relative error of at most 0.012.
Values may be sent and summed in bfloat16 or wider, within the bound.
A program may use at most 64 MiB of HBM per device.

```python
import math
import jax
import jax.numpy as jnp
import numpy as np
from jax import lax

STATIONS = 62
DIRS = 18
SRC = 20
T_DEV = 2
CHAN = 128
BASE = 480
TIMES = 4
INTERVALS = 2
N_TM = 2


def draw_baseline_stations(key, part):
    first_station, second_station = np.triu_indices(STATIONS, 1)
    pair_count = first_station.shape[0]
    shuffled = jax.random.permutation(key, pair_count)
    repeats = BASE // pair_count + 1
    chosen = jnp.tile(shuffled, repeats)[:BASE]
    first_column = jnp.asarray(first_station, dtype=jnp.int32)[chosen]
    second_column = jnp.asarray(second_station, dtype=jnp.int32)[chosen]
    return jnp.stack([first_column, second_column], axis=1)


def random_signs(key, shape):
    return jnp.where(jax.random.bernoulli(key, 0.5, shape), 1.0, -1.0).astype(jnp.float32)


def draw_baseline_coords(key, part):
    subkeys = jax.random.split(jax.random.fold_in(key, 11), 3)
    plane_shape = (2, TIMES, BASE)
    magnitude = jax.random.uniform(subkeys[0], plane_shape, jnp.float32, 150.0, 180.0)
    planar = magnitude * random_signs(subkeys[1], plane_shape)
    depths = jnp.clip(30.0 * jax.random.normal(subkeys[2], (1, TIMES, BASE), jnp.float32), -90.0, 90.0)
    return jnp.concatenate([planar, depths], axis=0)


def draw_source_offsets(key, part):
    subkeys = jax.random.split(jax.random.fold_in(key, 23), 2)
    magnitude = jax.random.uniform(subkeys[0], (2, SRC), jnp.float32, 0.06, 0.08)
    return magnitude * random_signs(subkeys[1], (2, SRC))


def channel_terms():
    channel_coord = (2.0 * jnp.arange(CHAN, dtype=jnp.int32).astype(jnp.float32) + 1.0) / CHAN - 1.0
    second_term = 1.5 * channel_coord * channel_coord - 0.5
    return (channel_coord.reshape(1, 1, CHAN, 1, 1), second_term.reshape(1, 1, CHAN, 1, 1))


def draw_local_gains(key, part):
    subkeys = jax.random.split(jax.random.fold_in(key, 37), 3)
    coeff_shape = (2, INTERVALS, 1, DIRS, STATIONS)
    full_shape = (2, INTERVALS, CHAN, DIRS, STATIONS)
    channel_coord, second_term = channel_terms()
    centre = jnp.array([0.8, 0.0], jnp.float32).reshape(2, 1, 1, 1, 1)
    slopes = jax.random.uniform(subkeys[0], coeff_shape, jnp.float32, -0.8, 0.8)
    curves = jax.random.uniform(subkeys[1], coeff_shape, jnp.float32, -0.3, 0.3)
    jitter = 0.08 * jax.random.normal(subkeys[2], full_shape, jnp.float32)
    values = centre + slopes * channel_coord + curves * second_term + jitter
    return jnp.clip(values, -1.6, 3.2)


def draw_dual_gains(key, part):
    subkeys = jax.random.split(jax.random.fold_in(key, 53), 4)
    coeff_shape = (2, INTERVALS, 1, DIRS, STATIONS)
    full_shape = (2, INTERVALS, CHAN, DIRS, STATIONS)
    channel_coord, second_term = channel_terms()
    signs = random_signs(subkeys[0], coeff_shape)
    strength = jax.random.uniform(subkeys[1], coeff_shape, jnp.float32, 1.5, 2.5)
    curves = jax.random.uniform(subkeys[2], coeff_shape, jnp.float32, -0.5, 0.5)
    jitter = 0.15 * jax.random.normal(subkeys[3], full_shape, jnp.float32)
    values = signs * strength * channel_coord + curves * second_term + jitter
    return jnp.clip(values, -3.5, 3.5)


def with_ends(values, stream_key, least, high):
    place = [jax.random.randint(jax.random.fold_in(stream_key, axis), (), 0, length) for axis, length in enumerate(values.shape)]
    widest = values.shape.index(max(values.shape))
    beside = place[:widest] + [(place[widest] + 1) % values.shape[widest]] + place[widest + 1:]
    return values.at[tuple(place)].set(least).at[tuple(beside)].set(high)


def levels(own_key, extent, cuts, least, largest):
    loudness = 1.0
    for dim, shards_of in cuts:
        draws = jax.random.uniform(jax.random.fold_in(jax.random.fold_in(own_key, 6), dim), (shards_of,), jnp.float32, least / len(cuts), largest / len(cuts))
        loudness = loudness * jnp.repeat(jnp.exp(draws), extent[dim] // shards_of).reshape((-1,) + (1,) * (len(extent) - 1 - dim))
    return loudness


def different_ones(rng, rows, number_of, top, lift):
    order = jax.random.permutation(jax.random.fold_in(rng, 1), number_of)
    boost = order
    for power in range(3):
        boost = boost * boost // number_of
    boost = boost * lift // number_of
    tickets = jax.random.randint(jax.random.fold_in(rng, 2), (rows, number_of), 0, 4096) + boost
    fixed_rows = jax.random.permutation(jax.random.fold_in(rng, 3), rows)[jnp.arange(number_of) % rows]
    tickets = jnp.where(jnp.arange(rows)[:, None] == fixed_rows[None, :], 1 << 14, tickets)
    merit = tickets * number_of + jnp.arange(number_of)
    return lax.top_k(merit.astype(jnp.int32), top)[1].astype(jnp.int32)


def normal_values(rng, shape, deviation, reach, cuts=(), held_as=jnp.bfloat16):
    loudness = levels(rng, shape, cuts, -0.22, 0.18) if cuts else 1.0
    result = jax.random.normal(rng, shape, jnp.float32) * deviation * loudness
    return jnp.minimum(jnp.maximum(result, -reach), reach).astype(held_as)


def setup_inputs(seed: int = 0) -> dict:
    arg_keys = jax.random.split(jax.random.key(seed), 11)
    return {
        "visibilities": normal_values(arg_keys[0], (2, TIMES, CHAN, BASE), 1.0, 6.0, ((1, 2), (2, 16))),
        "baseline_coords": draw_baseline_coords(jax.random.fold_in(arg_keys[10], 71), 0),
        "source_offsets": draw_source_offsets(jax.random.fold_in(arg_keys[10], 71), 0),
        "source_flux": jnp.clip(jnp.exp(math.log(0.1) - 2.3025851 * jax.random.uniform(arg_keys[3], (SRC, CHAN), jnp.float32) ** levels(arg_keys[3], (SRC, CHAN), ((1, 16),), -0.2, 0.2)), 0.01, 0.1),
        "cluster_of_source": different_ones(arg_keys[4], SRC, DIRS, 1, 0),
        "baseline_stations": draw_baseline_stations(jax.random.fold_in(arg_keys[10], 71), 0),
        "station_flags": with_ends((jax.random.randint(arg_keys[6], (STATIONS, TIMES), 0, 8) < 1).astype(jnp.int32), jax.random.fold_in(arg_keys[6], 1), 0, 1),
        "local_gains": draw_local_gains(jax.random.fold_in(arg_keys[10], 71), 0),
        "dual_gains": draw_dual_gains(jax.random.fold_in(arg_keys[10], 71), 0),
        "penalty": jnp.clip(jnp.exp(jax.random.uniform(arg_keys[9], (DIRS,), jnp.float32, math.log(0.4), math.log(0.8))), 0.4, 0.8),
    }


HIGHEST = lax.Precision.HIGHEST

def legendre_basis(indices, total):
    coordinate = (2 * indices + 1).astype(jnp.float32) / total - 1.0
    return jnp.stack([jnp.ones_like(coordinate), coordinate, 1.5 * coordinate * coordinate - 0.5], axis=1)

def channel_scale(indices, total):
    return 2.0 * math.pi * (0.9 + 0.2 * (indices.astype(jnp.float32) + 0.5) / total)

def blackman_taper(total):
    angles = 2.0 * math.pi / (total - 1) * jnp.arange(total, dtype=jnp.int32).astype(jnp.float32)
    return 0.35875 - 0.48829 * jnp.cos(angles) + 0.14128 * jnp.cos(2.0 * angles) - 0.01168 * jnp.cos(3.0 * angles)

def delay_table(total):
    indices = jnp.arange(total, dtype=jnp.int32)
    product = indices[:, None] * indices[None, :] % total
    angles = 2.0 * math.pi / total * product.astype(jnp.float32)
    return jnp.concatenate([jnp.cos(angles), jnp.sin(angles)], axis=1).astype(jnp.bfloat16)

def solve_gram(factor, right_side):
    middle = lax.linalg.triangular_solve(factor, right_side, left_side=True, lower=True)
    return lax.linalg.triangular_solve(factor, middle, left_side=True, lower=True, transpose_a=True)

def keep_weight(flags, first, second):
    return ((1.0 - jnp.take(flags, first, axis=0)) * (1.0 - jnp.take(flags, second, axis=0))).T

def source_model(coeffs, basis, first, second, onehot, flux, antenna_pair_coordinates, offsets, depth, scale):
    gain_first = jnp.einsum('fk,krdb->rfdb', basis, jnp.take(coeffs, first, axis=3), precision=HIGHEST)
    gain_second = jnp.einsum('fk,krdb->rfdb', basis, jnp.take(coeffs, second, axis=3), precision=HIGHEST)
    pair_real = gain_first[0] * gain_second[0] + gain_first[1] * gain_second[1]
    pair_imag = gain_first[1] * gain_second[0] - gain_first[0] * gain_second[1]
    coef_real = jnp.einsum('sd,fdb->sfb', onehot, pair_real, precision=HIGHEST) * flux[:, :, None]
    coef_imag = jnp.einsum('sd,fdb->sfb', onehot, pair_imag, precision=HIGHEST) * flux[:, :, None]
    lag_grid = offsets[0][:, None, None] * antenna_pair_coordinates[0][None] + offsets[1][:, None, None] * antenna_pair_coordinates[1][None] + depth[:, None, None] * antenna_pair_coordinates[2][None]
    sampling_epochs = antenna_pair_coordinates.shape[1]
    frequency_bins = coef_real.shape[1]
    pair_group_extent = coef_real.shape[2]

    def accumulate(carry, pieces):
        part_real, part_imag, part_delay = pieces
        angles = scale[None, :, None] * part_delay[:, None, :]
        cosine = jnp.cos(angles)
        sine_part = jnp.sin(angles)
        return ((carry[0] + (part_real[None] * cosine + part_imag[None] * sine_part), carry[1] + (part_imag[None] * cosine - part_real[None] * sine_part)), None)
    offset_first_entry = (jnp.zeros((sampling_epochs, frequency_bins, pair_group_extent), jnp.float32), jnp.zeros((sampling_epochs, frequency_bins, pair_group_extent), jnp.float32))
    (model_real, model_imag), unused = lax.scan(accumulate, offset_first_entry, (coef_real, coef_imag, lag_grid))
    return (model_real, model_imag)

def cross_terms(residual, taper, table, norm):
    tapered = (residual * taper[None, None, :, None]).astype(jnp.bfloat16)
    raw = jnp.einsum('rtcb,ck->rtbk', tapered.astype(jnp.float32), table.astype(jnp.float32), precision=HIGHEST)
    width = table.shape[1] // 2
    spec_real = (raw[0, :, :, :width] + raw[1, :, :, width:]) * norm
    spec_imag = (raw[1, :, :, :width] - raw[0, :, :, width:]) * norm
    halves = spec_real.shape[0] // 2
    paired_real = spec_real.reshape(halves, 2, spec_real.shape[1], spec_real.shape[2])
    paired_imag = spec_imag.reshape(halves, 2, spec_imag.shape[1], spec_imag.shape[2])
    return lax.optimization_barrier(jnp.sum(paired_real[:, 0] * paired_real[:, 1] + paired_imag[:, 0] * paired_imag[:, 1], axis=0))

def reference(visibilities, baseline_coords, source_offsets, source_flux, cluster_of_source, baseline_stations, station_flags, local_gains, dual_gains, penalty):
    all_index = jnp.arange(CHAN, dtype=jnp.int32)
    basis = legendre_basis(all_index, CHAN)
    factor = jnp.linalg.cholesky(jnp.dot(basis.T, basis, precision=HIGHEST))
    scale = channel_scale(all_index, CHAN)
    taper = blackman_taper(CHAN)
    table = delay_table(CHAN)
    norm = 1.0 / jnp.sqrt(jnp.sum(taper * taper))
    rate = penalty[:, None]
    onehot = (cluster_of_source == jnp.arange(DIRS, dtype=jnp.int32)[None, :]).astype(jnp.float32)
    depth = jnp.sqrt(1.0 - source_offsets[0] * source_offsets[0] - source_offsets[1] * source_offsets[1]) - 1.0
    first = baseline_stations[:, 0]
    second = baseline_stations[:, 1]
    flag_float = station_flags.astype(jnp.float32)

    def interval(which):
        local_now = lax.dynamic_index_in_dim(local_gains, which, 1, keepdims=False)
        dual_now = lax.dynamic_index_in_dim(dual_gains, which, 1, keepdims=False)
        target = local_now + dual_now / rate
        totals = jnp.einsum('fk,rfdp->krdp', basis, target, precision=HIGHEST)
        coeffs = solve_gram(factor, totals.reshape(totals.shape[0], -1)).reshape(totals.shape)
        smooth = jnp.einsum('fk,krdp->rfdp', basis, coeffs, precision=HIGHEST)
        dual_next = dual_now + rate * (local_now - smooth)
        offset_first_entry = (which * T_DEV).astype(jnp.int32)
        antenna_pair_coordinates = lax.dynamic_slice_in_dim(baseline_coords, offset_first_entry, T_DEV, 1)
        flags_now = lax.dynamic_slice_in_dim(flag_float, offset_first_entry, T_DEV, 1)
        vis_now = lax.dynamic_slice_in_dim(visibilities, offset_first_entry, T_DEV, 1)
        model_real, model_imag = source_model(coeffs, basis, first, second, onehot, source_flux, antenna_pair_coordinates, source_offsets, depth, scale)
        keep = keep_weight(flags_now, first, second)
        residual = (keep[None, :, None, :] * (vis_now - jnp.stack([model_real, model_imag]))).astype(jnp.bfloat16)
        return (cross_terms(residual, taper, table, norm), dual_next)
    cross_all, dual_all = lax.map(interval, jnp.arange(N_TM, dtype=jnp.int32))
    cross_power = lax.optimization_barrier(jnp.sum(cross_all, axis=0)) / (TIMES // 2)
    dual_update = jnp.moveaxis(dual_all, 0, 1)
    return (cross_power, dual_update)
```

```python
import math

import jax
import jax.numpy as jnp
import numpy as np
from jax import lax
from jax.experimental import pallas as pl
from jax.experimental.pallas import tpu as pltpu
from jax.sharding import PartitionSpec as P

HIGHEST = lax.Precision.HIGHEST
MESH = pl.DeviceIdType.MESH
TERMS = 3
F32 = jnp.float32
BF16 = jnp.bfloat16


def turn_polynomials():
    nodes = np.cos(np.pi * (np.arange(400) + 0.5) / 400) * 0.125 + 0.125
    root = np.sqrt(nodes)
    cosine = np.polynomial.Chebyshev.fit(nodes, np.cos(2 * np.pi * root), 6)
    sine = np.polynomial.Chebyshev.fit(nodes, np.sin(2 * np.pi * root) / root, 6)
    pick = lambda fit: [float(c) for c in fit.convert(kind=np.polynomial.Polynomial).coef]
    return pick(cosine), pick(sine)


COS_TERMS, SIN_TERMS = turn_polynomials()


def horner(terms, z):
    value = jnp.full_like(z, terms[-1])
    for term in terms[-2::-1]:
        value = value * z + term
    return value


def taper_values(total):
    angles = 2.0 * np.pi / (total - 1) * np.arange(total)
    return 0.35875 - 0.48829 * np.cos(angles) + 0.14128 * np.cos(2 * angles) - 0.01168 * np.cos(3 * angles)


def delay_tables(total, parts):
    index = np.arange(total)
    angles = 2.0 * np.pi / total * (index[:, None] * index[None, :] % total)
    wide = total // parts
    cosine = np.cos(angles).reshape(total, parts, wide)
    sine = np.sin(angles).reshape(total, parts, wide)
    return jnp.asarray(np.concatenate([cosine, sine], axis=2).transpose(1, 0, 2), BF16)


def gram_inverse(total):
    x = (2.0 * np.arange(total) + 1.0) / total - 1.0
    basis = np.stack([np.ones_like(x), x, 1.5 * x * x - 0.5], axis=1)
    return np.linalg.inv(basis.T @ basis)


def ceil_to(value, step):
    return -(-value // step) * step


def split_groups(groups):
    low = 1
    while low * 2 * low * 2 <= groups and groups % (low * 2) == 0:
        low *= 2
    return low, groups // low


def iota(shape, dim):
    return lax.broadcasted_iota(jnp.int32, shape, dim)


def make_kernel(cfg):
    groups, parts, width, dirs, stations = (cfg[k] for k in ("groups", "parts", "width", "dirs", "stations"))
    sources, epochs, base, own, pad = (cfg[k] for k in ("sources", "epochs", "base", "own", "pad"))
    low, high, rows, total = (cfg[k] for k in ("low", "high", "rows", "total"))
    count = groups * parts
    lanes = groups * pad
    half = cfg["half"]
    inverse = gram_inverse(total)
    norm2 = 1.0 / float(np.sum(taper_values(total) ** 2))
    pair_total = (epochs // 2) * parts
    slab = 2 * epochs * pad
    per_tile = 128 // pad

    def kernel(
        cluster, vis, coords, offsets, flux, pairs, flags, local, dual, penalty, taper, table,
        cross_out, dual_out,
        packed, sum_send, sum_recv, part_send, part_recv, perm, onehot, delay, wave_c, wave_s,
        pair_r, pair_i, out_send, out_recv,
        s1_send, s1_recv, s2_send, s2_recv, a_send, a_recv,
    ):
        chan = lax.axis_index("chan")
        part = lax.axis_index("tm")
        me = part * groups + chan
        barrier = pltpu.get_barrier_semaphore()

        def others(act):
            for dm in range(parts):
                m = lax.rem(part + dm, parts)

                def step(i, carry, m=m):
                    act(lax.rem(chan + i, groups), m)
                    return carry

                first = 1 if dm == 0 else 0
                lax.fori_loop(first, groups, step, 0, unroll=groups <= 16)

        others(lambda c, m: pl.semaphore_signal(barrier, inc=1, device_id={"chan": c, "tm": m}, device_id_type=MESH))

        tall = dirs * width
        rate = jnp.sum(
            jnp.where(iota((tall, dirs), 0) // width == iota((tall, dirs), 1), penalty[...], 0.0), axis=1, keepdims=True
        )
        packed[...] = jnp.zeros_like(packed)
        inverse_rate = 1.0 / rate
        for r in range(2):
            packed[:, r * half : r * half + stations] = local[r] + dual[r] * inverse_rate

        def coordinate(f):
            return (2 * (chan * width + f) + 1).astype(F32) / total - 1.0

        def term_of(row):
            k = sum((row >= dirs * i).astype(jnp.int32) for i in range(1, TERMS + 1))
            return k, row - k * dirs

        row, col = iota((rows, tall), 0), iota((rows, tall), 1)
        k, d = term_of(row)
        x = coordinate(lax.rem(col, width))
        value = jnp.where(k == 0, 1.0, jnp.where(k == 1, x, 1.5 * x * x - 0.5))
        weights = jnp.where((d == col // width) & (k < TERMS), value, 0.0)
        sum_send[...] = jnp.dot(weights, packed[...], precision=HIGHEST, preferred_element_type=F32)

        lo, hi = lax.rem(chan, low), chan // low
        pl.semaphore_wait(barrier, count - 1)

        def stage(src, dst, send, recv, size, mine, address):
            copies = []
            for i in range(1, size):
                copies.append(
                    pltpu.make_async_remote_copy(
                        src_ref=src,
                        dst_ref=dst.at[i - 1],
                        send_sem=send.at[i - 1],
                        recv_sem=recv.at[i - 1],
                        device_id={"chan": address(lax.rem(mine + i, size)), "tm": part},
                        device_id_type=MESH,
                    )
                )
            for copy in copies:
                copy.start()
            return copies

        first = stage(sum_send, sum_recv, s1_send, s1_recv, low, lo, lambda t: hi * low + t)

        prow, pcol = iota((base, lanes), 0), iota((base, lanes), 1)
        inner = lax.rem(pcol, pad)
        perm[...] = jnp.where((prow == (pcol // pad) * own + inner) & (inner < own), 1.0, 0.0).astype(BF16)
        place = perm[...]
        station_rows = jnp.dot(pairs[...].astype(F32).astype(BF16), place, preferred_element_type=F32).astype(jnp.int32)
        srow = iota((2 * half, lanes), 0)
        for side in range(2):
            line = station_rows[side : side + 1, :]
            for r in range(2):
                onehot[r, :, side * lanes : (side + 1) * lanes] = jnp.where(srow == line + r * half, 1.0, 0.0).astype(BF16)

        def placed(value):
            out = None
            for _ in range(3):
                piece = value.astype(BF16)
                value = value - piece.astype(F32)
                moved = jnp.dot(piece, place, preferred_element_type=F32)
                out = moved if out is None else out + moved
            return out

        u, v, w = (placed(coords[i]) for i in range(3))
        same = iota((sources, sources), 0) == iota((sources, sources), 1)
        column = lambda line: jnp.sum(jnp.where(same, line, 0.0), axis=1, keepdims=True)
        l, m = offsets[0:1, :], offsets[1:2, :]
        lc, mc, nc = column(l), column(m), column(jnp.sqrt(1.0 - l * l - m * m) - 1.0)
        for t in range(epochs):
            delay[t] = lc * u[t : t + 1] + mc * v[t : t + 1] + nc * w[t : t + 1]
        vis_placed = [
            [jnp.dot(vis[r, t].astype(F32).astype(BF16), place, preferred_element_type=F32) for t in range(epochs)]
            for r in range(2)
        ]
        unflagged = (1.0 - flags[...].astype(F32)).astype(BF16)
        kept = jnp.dot(unflagged, onehot[0, 0:stations, :], preferred_element_type=F32)
        keep = kept[:, :lanes] * kept[:, lanes:]
        channel = (chan * width + iota((width, 1), 0)).astype(F32)
        rate_turns = 0.9 + 0.2 * (channel + 0.5) / total

        def phases(begin, end):
            for s in range(begin, end):
                scale = flux[:, s : s + 1]
                for t in range(epochs):
                    turns = rate_turns * delay[t, s : s + 1, :]
                    turns = turns - jnp.round(turns)
                    z = turns * turns
                    wave_c[s, t] = scale * horner(COS_TERMS, z)
                    wave_s[s, t] = scale * (turns * horner(SIN_TERMS, z))

        phases(0, sources // 2)
        acc = sum_send[...]
        for i, copy in enumerate(first):
            copy.wait_recv()
            acc = acc + sum_recv[i]
        part_send[...] = acc
        second = stage(part_send, part_recv, s2_send, s2_recv, high, hi, lambda t: t * low + lo)
        phases(sources // 2, sources)
        vrow, vcol = iota((tall, rows), 0), iota((tall, rows), 1)
        k, d = term_of(vcol)
        x = coordinate(lax.rem(vrow, width))
        x2 = 1.5 * x * x - 0.5
        value = jnp.zeros_like(x)
        for i in range(TERMS):
            mixed = float(inverse[0, i]) + x * float(inverse[1, i]) + x2 * float(inverse[2, i])
            value = jnp.where(k == i, mixed, value)
        spread = jnp.where((d == vrow // width) & (k < TERMS), value, 0.0)
        for i, copy in enumerate(second):
            copy.wait_recv()
            acc = acc + part_recv[i]

        smooth = jnp.dot(spread, acc, precision=HIGHEST, preferred_element_type=F32)
        big = smooth.astype(BF16)
        small = (smooth - big.astype(F32)).astype(BF16)
        gains = [
            jnp.dot(big, onehot[r], preferred_element_type=F32) + jnp.dot(small, onehot[r], preferred_element_type=F32)
            for r in range(2)
        ]
        for d in range(dirs):
            band = slice(d * width, (d + 1) * width)
            pr, pi = gains[0][band, :lanes], gains[1][band, :lanes]
            qr, qi = gains[0][band, lanes:], gains[1][band, lanes:]
            pair_r[d] = pr * qr + pi * qi
            pair_i[d] = pi * qr - pr * qi
        model_r = [jnp.zeros((width, lanes), F32) for _ in range(epochs)]
        model_i = [jnp.zeros((width, lanes), F32) for _ in range(epochs)]
        for s in range(sources):
            which = cluster[s]
            gr, gi = pair_r[which], pair_i[which]
            for t in range(epochs):
                c, n = wave_c[s, t], wave_s[s, t]
                model_r[t] = model_r[t] + (gr * c + gi * n)
                model_i[t] = model_i[t] + (gi * c - gr * n)
        window = taper[chan]
        tiles = []
        for r in range(2):
            for t in range(epochs):
                left = vis_placed[r][t] - (model_r[t] if r == 0 else model_i[t])
                left = (keep[t : t + 1, :] * left).astype(BF16).astype(F32)
                tiles.append((left * window[:, 0:1]).astype(BF16).astype(F32))
        slot = iota((width, 128), 1) // pad
        for c in range(groups):
            tile, place_in = c // per_tile, c % per_tile
            for start in range(0, len(tiles), per_tile):
                block = None
                for j in range(per_tile):
                    piece = tiles[start + j][:, tile * 128 : (tile + 1) * 128]
                    shift = ((j - place_in) * pad) % 128
                    piece = pltpu.roll(piece, shift, 1) if shift else piece
                    block = piece if block is None else jnp.where(slot == j, piece, block)
                out_send[c, :, start * pad : start * pad + 128] = block.astype(BF16)
        out_recv[me] = out_send[chan]

        def push(c, m):
            return pltpu.make_async_remote_copy(
                src_ref=out_send.at[c],
                dst_ref=out_recv.at[me],
                send_sem=a_send,
                recv_sem=a_recv,
                device_id={"chan": c, "tm": m},
                device_id_type=MESH,
            )

        others(lambda c, m: push(c, m).start())

        for r in range(2):
            dual_out[r] = dual[r] + rate * (local[r] - smooth[:, r * half : r * half + stations])
        for copy in first + second:
            copy.wait_send()

        whole = pltpu.make_async_remote_copy(
            src_ref=out_recv.at[pl.ds(0, count - 1)],
            dst_ref=out_recv.at[pl.ds(0, count - 1)],
            send_sem=a_send,
            recv_sem=a_recv,
            device_id={"chan": lax.rem(chan + 1, groups), "tm": part},
            device_id_type=MESH,
        )
        whole.wait_recv()
        wide = total // parts
        kernel_table = table[part]
        cross = jnp.zeros((pad, wide), F32)
        for m in range(parts):
            grid = out_recv[m * groups : (m + 1) * groups].astype(F32).reshape(total, slab)
            raw = jnp.dot(grid.T.astype(BF16), kernel_table, preferred_element_type=F32)
            rest = epochs * pad
            real = raw[:rest, :wide] + raw[rest:, wide:]
            imag = raw[rest:, :wide] - raw[:rest, wide:]
            for j in range(epochs // 2):
                a, b = slice(2 * j * pad, (2 * j + 1) * pad), slice((2 * j + 1) * pad, (2 * j + 2) * pad)
                cross = cross + (real[a] * real[b] + imag[a] * imag[b])
        cross_out[...] = cross[:own] * (norm2 / pair_total)
        whole.wait_send()

    return kernel


def shards(
    visibilities, baseline_coords, source_offsets, source_flux, cluster_of_source,
    baseline_stations, station_flags, local_gains, dual_gains, penalty,
):
    groups, parts = lax.axis_size("chan"), lax.axis_size("tm")
    sources, width = source_flux.shape
    _, epochs, _, base = visibilities.shape
    _, _, _, dirs, stations = local_gains.shape
    total = width * groups
    own = base // groups
    pad = ceil_to(own, 32)
    lanes = groups * pad
    half = ceil_to(stations, 64)
    rows = ceil_to(TERMS * dirs, 8)
    low, high = split_groups(groups)
    tall = dirs * width
    slab = 2 * epochs * pad
    count = groups * parts
    cfg = dict(
        groups=groups, parts=parts, width=width, dirs=dirs, stations=stations, sources=sources, epochs=epochs,
        base=base, own=own, pad=pad, low=low, high=high, rows=rows, total=total, half=half,
    )
    taper = jnp.asarray(np.broadcast_to(taper_values(total).reshape(groups, width, 1), (groups, width, 128)), F32)
    table = delay_tables(total, parts)
    turned = lambda a: a[:, 0].transpose(0, 2, 1, 3).reshape(2, tall, stations)
    vmem = pl.BlockSpec(memory_space=pltpu.VMEM)
    cross, dual = pl.pallas_call(
        make_kernel(cfg),
        out_shape=(
            jax.ShapeDtypeStruct((own, total // parts), F32),
            jax.ShapeDtypeStruct((2, tall, stations), F32),
        ),
        in_specs=[pl.BlockSpec(memory_space=pltpu.SMEM)] + [vmem] * 11,
        out_specs=(vmem, vmem),
        scratch_shapes=[
            pltpu.VMEM((tall, 2 * half), F32),
            pltpu.VMEM((rows, 2 * half), F32),
            pltpu.VMEM((max(low - 1, 1), rows, 2 * half), F32),
            pltpu.VMEM((rows, 2 * half), F32),
            pltpu.VMEM((max(high - 1, 1), rows, 2 * half), F32),
            pltpu.VMEM((base, lanes), BF16),
            pltpu.VMEM((2, 2 * half, 2 * lanes), BF16),
            pltpu.VMEM((epochs, sources, lanes), F32),
            pltpu.VMEM((sources, epochs, width, lanes), F32),
            pltpu.VMEM((sources, epochs, width, lanes), F32),
            pltpu.VMEM((dirs, width, lanes), F32),
            pltpu.VMEM((dirs, width, lanes), F32),
            pltpu.VMEM((groups, width, slab), BF16),
            pltpu.VMEM((count, width, slab), BF16),
            pltpu.SemaphoreType.DMA((max(low - 1, 1),)),
            pltpu.SemaphoreType.DMA((max(low - 1, 1),)),
            pltpu.SemaphoreType.DMA((max(high - 1, 1),)),
            pltpu.SemaphoreType.DMA((max(high - 1, 1),)),
            pltpu.SemaphoreType.DMA,
            pltpu.SemaphoreType.DMA,
        ],
        compiler_params=pltpu.CompilerParams(
            collective_id=0, has_side_effects=True, vmem_limit_bytes=60 * 1024 * 1024
        ),
    )(
        cluster_of_source.reshape(sources), visibilities, baseline_coords, source_offsets, source_flux.T,
        baseline_stations.T, station_flags.T, turned(local_gains), turned(dual_gains), penalty.reshape(1, dirs),
        taper, table,
    )
    dual = dual.reshape(2, dirs, width, stations).transpose(0, 2, 1, 3)[:, None]
    return (cross, dual)


def solution(mesh):
    in_specs = (
        P(None, "tm", "chan", None),
        P(None, "tm", None),
        P(),
        P(None, "chan"),
        P(),
        P(),
        P(None, "tm"),
        P(None, "tm", "chan", None, None),
        P(None, "tm", "chan", None, None),
        P(),
    )
    out_specs = (P("chan", "tm"), P(None, "tm", "chan", None, None))
    return jax.shard_map(shards, mesh=mesh, in_specs=in_specs, out_specs=out_specs, check_vma=False)
```

```python
import math

import jax
import jax.numpy as jnp
import numpy as np
from jax import lax
from jax.experimental import pallas as pl
from jax.experimental.pallas import tpu as pltpu
from jax.sharding import PartitionSpec as P

HIGHEST = lax.Precision.HIGHEST
MESH = pl.DeviceIdType.MESH
TERMS = 3
F32 = jnp.float32
BF16 = jnp.bfloat16


def turn_polynomials():
    nodes = np.cos(np.pi * (np.arange(400) + 0.5) / 400) * 0.125 + 0.125
    root = np.sqrt(nodes)
    cosine = np.polynomial.Chebyshev.fit(nodes, np.cos(2 * np.pi * root), 6)
    sine = np.polynomial.Chebyshev.fit(nodes, np.sin(2 * np.pi * root) / root, 6)
    pick = lambda fit: [float(c) for c in fit.convert(kind=np.polynomial.Polynomial).coef]
    return pick(cosine), pick(sine)


COS_TERMS, SIN_TERMS = turn_polynomials()


def horner(terms, z):
    value = jnp.full_like(z, terms[-1])
    for term in terms[-2::-1]:
        value = value * z + term
    return value


def taper_values(total):
    angles = 2.0 * np.pi / (total - 1) * np.arange(total)
    return 0.35875 - 0.48829 * np.cos(angles) + 0.14128 * np.cos(2 * angles) - 0.01168 * np.cos(3 * angles)


def delay_tables(total, parts):
    index = np.arange(total)
    angles = 2.0 * np.pi / total * (index[:, None] * index[None, :] % total)
    wide = total // parts
    cosine = np.cos(angles).reshape(total, parts, wide)
    sine = np.sin(angles).reshape(total, parts, wide)
    return jnp.asarray(np.concatenate([cosine, sine], axis=2).transpose(1, 0, 2), BF16)


def gram_inverse(total):
    x = (2.0 * np.arange(total) + 1.0) / total - 1.0
    basis = np.stack([np.ones_like(x), x, 1.5 * x * x - 0.5], axis=1)
    return np.linalg.inv(basis.T @ basis)


def ceil_to(value, step):
    return -(-value // step) * step


def split_groups(groups):
    low = 1
    while low * 2 * low * 2 <= groups and groups % (low * 2) == 0:
        low *= 2
    return low, groups // low


def iota(shape, dim):
    return lax.broadcasted_iota(jnp.int32, shape, dim)


def make_kernel(cfg):
    groups, parts, width, dirs, stations = (cfg[k] for k in ("groups", "parts", "width", "dirs", "stations"))
    sources, epochs, base, own, pad = (cfg[k] for k in ("sources", "epochs", "base", "own", "pad"))
    low, high, rows, total = (cfg[k] for k in ("low", "high", "rows", "total"))
    count = groups * parts
    lanes = groups * pad
    half = cfg["half"]
    inverse = gram_inverse(total)
    norm2 = 1.0 / float(np.sum(taper_values(total) ** 2))
    pair_total = (epochs // 2) * parts
    slab = 2 * epochs * pad
    per_tile = 128 // pad

    def kernel(
        cluster_hbm, vis_hbm, coords_hbm, offsets_hbm, flux_hbm, pairs_hbm, flags_hbm, local_hbm, dual_hbm,
        penalty_hbm, taper_hbm, table_hbm,
        cross_out, dual_out,
        cluster, vis, coords, offsets, flux, pairs, flags, local, dual, penalty, window_buf, table_buf, load_sem,
        packed, sum_send, sum_recv, part_send, part_recv, perm, onehot, delay, wave_c, wave_s,
        pair_r, pair_i, out_send, out_recv,
        s1_send, s1_recv, s2_send, s2_recv, a_send, a_recv,
    ):
        chan = lax.axis_index("chan")
        part = lax.axis_index("tm")
        me = part * groups + chan
        barrier = pltpu.get_barrier_semaphore()

        def others(act):
            for dm in range(parts):
                m = lax.rem(part + dm, parts)

                def step(i, carry, m=m):
                    act(lax.rem(chan + i, groups), m)
                    return carry

                first = 1 if dm == 0 else 0
                lax.fori_loop(first, groups, step, 0, unroll=groups <= 16)

        lo, hi = lax.rem(chan, low), chan // low

        def greet(c, m):
            pl.semaphore_signal(barrier, inc=1, device_id={"chan": c, "tm": m}, device_id_type=MESH)

        for i in range(1, high):
            greet(lax.rem(hi + i, high) * low + lo, part)
        for i in range(1, low):
            greet(hi * low + lax.rem(lo + i, low), part)
        for i in range(1, parts):
            greet(chan, lax.rem(part + i, parts))
        loads = [
            pltpu.make_async_copy(src, dst, load_sem.at[i])
            for i, (src, dst) in enumerate(
                [
                    (penalty_hbm, penalty), (dual_hbm, dual), (local_hbm, local), (pairs_hbm, pairs),
                    (coords_hbm, coords), (offsets_hbm, offsets), (flux_hbm, flux), (flags_hbm, flags),
                    (vis_hbm, vis), (taper_hbm.at[chan], window_buf), (table_hbm.at[part], table_buf),
                    (cluster_hbm, cluster),
                ]
            )
        ]
        for load in loads:
            load.start()

        tall = dirs * width

        def coordinate(f):
            return (2 * (chan * width + f) + 1).astype(F32) / total - 1.0

        def term_of(row):
            k = sum((row >= dirs * i).astype(jnp.int32) for i in range(1, TERMS + 1))
            return k, row - k * dirs

        row, col = iota((rows, tall), 0), iota((rows, tall), 1)
        k, d = term_of(row)
        x = coordinate(lax.rem(col, width))
        value = jnp.where(k == 0, 1.0, jnp.where(k == 1, x, 1.5 * x * x - 0.5))
        weights = jnp.where((d == col // width) & (k < TERMS), value, 0.0)
        prow, pcol = iota((base, lanes), 0), iota((base, lanes), 1)
        inner = lax.rem(pcol, pad)
        perm[...] = jnp.where((prow == (pcol // pad) * own + inner) & (inner < own), 1.0, 0.0).astype(BF16)
        packed[...] = jnp.zeros_like(packed)
        for load in loads[:3]:
            load.wait()
        rate = jnp.sum(
            jnp.where(iota((tall, dirs), 0) // width == iota((tall, dirs), 1), penalty[...], 0.0), axis=1, keepdims=True
        )
        inverse_rate = 1.0 / rate
        for r in range(2):
            packed[:, r * half : r * half + stations] = local[r] + dual[r] * inverse_rate

        acc = jnp.dot(weights, packed[...], precision=HIGHEST, preferred_element_type=F32)
        sum_send[...] = acc
        pl.semaphore_wait(barrier, low + high + parts - 3)

        def stage(src, dst, send, recv, size, mine, address):
            copies = []
            for i in range(1, size):
                copies.append(
                    pltpu.make_async_remote_copy(
                        src_ref=src,
                        dst_ref=dst.at[i - 1],
                        send_sem=send.at[i - 1],
                        recv_sem=recv.at[i - 1],
                        device_id={"chan": address(lax.rem(mine + i, size)), "tm": part},
                        device_id_type=MESH,
                    )
                )
            for copy in copies:
                copy.start()
            return copies

        first = stage(sum_send, sum_recv, s1_send, s1_recv, low, lo, lambda t: hi * low + t)
        for load in loads[3:]:
            load.wait()
        place = perm[...]
        station_rows = jnp.dot(pairs[...].astype(F32).astype(BF16), place, preferred_element_type=F32).astype(jnp.int32)
        srow = iota((2 * half, lanes), 0)
        for side in range(2):
            line = station_rows[side : side + 1, :]
            for r in range(2):
                onehot[r, :, side * lanes : (side + 1) * lanes] = jnp.where(srow == line + r * half, 1.0, 0.0).astype(BF16)

        def placed(value):
            out = None
            for _ in range(3):
                piece = value.astype(BF16)
                value = value - piece.astype(F32)
                moved = jnp.dot(piece, place, preferred_element_type=F32)
                out = moved if out is None else out + moved
            return out

        u, v, w = (placed(coords[i]) for i in range(3))
        same = iota((sources, sources), 0) == iota((sources, sources), 1)
        column = lambda line: jnp.sum(jnp.where(same, line, 0.0), axis=1, keepdims=True)
        l, m = offsets[0:1, :], offsets[1:2, :]
        lc, mc, nc = column(l), column(m), column(jnp.sqrt(1.0 - l * l - m * m) - 1.0)
        for t in range(epochs):
            delay[t] = lc * u[t : t + 1] + mc * v[t : t + 1] + nc * w[t : t + 1]
        vis_placed = [
            [jnp.dot(vis[r, t].astype(F32).astype(BF16), place, preferred_element_type=F32) for t in range(epochs)]
            for r in range(2)
        ]
        unflagged = (1.0 - flags[...].astype(F32)).astype(BF16)
        kept = jnp.dot(unflagged, onehot[0, 0:stations, :], preferred_element_type=F32)
        keep = kept[:, :lanes] * kept[:, lanes:]
        channel = (chan * width + iota((width, 1), 0)).astype(F32)
        rate_turns = 0.9 + 0.2 * (channel + 0.5) / total

        def phases(begin, end):
            for s in range(begin, end):
                scale = flux[:, s : s + 1]
                for t in range(epochs):
                    turns = rate_turns * delay[t, s : s + 1, :]
                    turns = turns - jnp.round(turns)
                    z = turns * turns
                    wave_c[s, t] = scale * horner(COS_TERMS, z)
                    wave_s[s, t] = scale * (turns * horner(SIN_TERMS, z))

        phases(0, sources // 2)
        for i, copy in enumerate(first):
            copy.wait_recv()
            acc = acc + sum_recv[i]
        part_send[...] = acc
        second = stage(part_send, part_recv, s2_send, s2_recv, high, hi, lambda t: t * low + lo)
        phases(sources // 2, sources)
        vrow, vcol = iota((tall, rows), 0), iota((tall, rows), 1)
        k, d = term_of(vcol)
        x = coordinate(lax.rem(vrow, width))
        x2 = 1.5 * x * x - 0.5
        value = jnp.zeros_like(x)
        for i in range(TERMS):
            mixed = float(inverse[0, i]) + x * float(inverse[1, i]) + x2 * float(inverse[2, i])
            value = jnp.where(k == i, mixed, value)
        spread = jnp.where((d == vrow // width) & (k < TERMS), value, 0.0)
        for i, copy in enumerate(second):
            copy.wait_recv()
            acc = acc + part_recv[i]

        smooth = jnp.dot(spread, acc, precision=HIGHEST, preferred_element_type=F32)
        big = smooth.astype(BF16)
        small = (smooth - big.astype(F32)).astype(BF16)
        gains = [
            jnp.dot(big, onehot[r], preferred_element_type=F32) + jnp.dot(small, onehot[r], preferred_element_type=F32)
            for r in range(2)
        ]
        for d in range(dirs):
            band = slice(d * width, (d + 1) * width)
            pr, pi = gains[0][band, :lanes], gains[1][band, :lanes]
            qr, qi = gains[0][band, lanes:], gains[1][band, lanes:]
            pair_r[d] = pr * qr + pi * qi
            pair_i[d] = pi * qr - pr * qi
        model_r = [jnp.zeros((width, lanes), F32) for _ in range(epochs)]
        model_i = [jnp.zeros((width, lanes), F32) for _ in range(epochs)]
        for s in range(sources):
            which = cluster[s]
            gr, gi = pair_r[which], pair_i[which]
            for t in range(epochs):
                c, n = wave_c[s, t], wave_s[s, t]
                model_r[t] = model_r[t] + (gr * c + gi * n)
                model_i[t] = model_i[t] + (gi * c - gr * n)
        window = window_buf[...]
        tiles = []
        for r in range(2):
            for t in range(epochs):
                left = vis_placed[r][t] - (model_r[t] if r == 0 else model_i[t])
                left = (keep[t : t + 1, :] * left).astype(BF16).astype(F32)
                tiles.append((left * window[:, 0:1]).astype(BF16).astype(F32))
        slot = iota((width, 128), 1) // pad
        for c in range(groups):
            tile, place_in = c // per_tile, c % per_tile
            for start in range(0, len(tiles), per_tile):
                block = None
                for j in range(per_tile):
                    piece = tiles[start + j][:, tile * 128 : (tile + 1) * 128]
                    shift = ((j - place_in) * pad) % 128
                    piece = pltpu.roll(piece, shift, 1) if shift else piece
                    block = piece if block is None else jnp.where(slot == j, piece, block)
                out_send[c, :, start * pad : start * pad + 128] = block.astype(BF16)
        out_recv[me] = out_send[chan]

        def push(c, m):
            return pltpu.make_async_remote_copy(
                src_ref=out_send.at[c],
                dst_ref=out_recv.at[me],
                send_sem=a_send,
                recv_sem=a_recv,
                device_id={"chan": c, "tm": m},
                device_id_type=MESH,
            )

        others(lambda c, m: push(c, m).start())

        for r in range(2):
            dual_out[r] = dual[r] + rate * (local[r] - smooth[:, r * half : r * half + stations])
        for copy in first + second:
            copy.wait_send()

        whole = pltpu.make_async_remote_copy(
            src_ref=out_recv.at[pl.ds(0, count - 1)],
            dst_ref=out_recv.at[pl.ds(0, count - 1)],
            send_sem=a_send,
            recv_sem=a_recv,
            device_id={"chan": lax.rem(chan + 1, groups), "tm": part},
            device_id_type=MESH,
        )
        whole.wait_recv()
        wide = total // parts
        kernel_table = table_buf[...]
        cross = jnp.zeros((pad, wide), F32)
        for m in range(parts):
            grid = out_recv[m * groups : (m + 1) * groups].astype(F32).reshape(total, slab)
            raw = jnp.dot(grid.T.astype(BF16), kernel_table, preferred_element_type=F32)
            rest = epochs * pad
            real = raw[:rest, :wide] + raw[rest:, wide:]
            imag = raw[rest:, :wide] - raw[:rest, wide:]
            for j in range(epochs // 2):
                a, b = slice(2 * j * pad, (2 * j + 1) * pad), slice((2 * j + 1) * pad, (2 * j + 2) * pad)
                cross = cross + (real[a] * real[b] + imag[a] * imag[b])
        cross_out[...] = cross[:own] * (norm2 / pair_total)
        whole.wait_send()

    return kernel


def shards(
    visibilities, baseline_coords, source_offsets, source_flux, cluster_of_source,
    baseline_stations, station_flags, local_gains, dual_gains, penalty,
):
    groups, parts = lax.axis_size("chan"), lax.axis_size("tm")
    sources, width = source_flux.shape
    _, epochs, _, base = visibilities.shape
    _, _, _, dirs, stations = local_gains.shape
    total = width * groups
    own = base // groups
    pad = ceil_to(own, 32)
    lanes = groups * pad
    half = ceil_to(stations, 64)
    rows = ceil_to(TERMS * dirs, 8)
    low, high = split_groups(groups)
    tall = dirs * width
    slab = 2 * epochs * pad
    count = groups * parts
    cfg = dict(
        groups=groups, parts=parts, width=width, dirs=dirs, stations=stations, sources=sources, epochs=epochs,
        base=base, own=own, pad=pad, low=low, high=high, rows=rows, total=total, half=half,
    )
    taper = jnp.asarray(np.broadcast_to(taper_values(total).reshape(groups, width, 1), (groups, width, 128)), F32)
    table = delay_tables(total, parts)
    turned = lambda a: a[:, 0].transpose(0, 2, 1, 3).reshape(2, tall, stations)
    vmem = pl.BlockSpec(memory_space=pltpu.VMEM)
    cross, dual = pl.pallas_call(
        make_kernel(cfg),
        out_shape=(
            jax.ShapeDtypeStruct((own, total // parts), F32),
            jax.ShapeDtypeStruct((2, tall, stations), F32),
        ),
        in_specs=[pl.BlockSpec(memory_space=pltpu.HBM)] * 12,
        out_specs=(vmem, vmem),
        scratch_shapes=[
            pltpu.SMEM((sources,), jnp.int32),
            pltpu.VMEM(visibilities.shape, BF16),
            pltpu.VMEM(baseline_coords.shape, F32),
            pltpu.VMEM(source_offsets.shape, F32),
            pltpu.VMEM((width, sources), F32),
            pltpu.VMEM((2, base), jnp.int32),
            pltpu.VMEM((epochs, stations), jnp.int32),
            pltpu.VMEM((2, tall, stations), F32),
            pltpu.VMEM((2, tall, stations), F32),
            pltpu.VMEM((1, dirs), F32),
            pltpu.VMEM((width, 128), F32),
            pltpu.VMEM((total, 2 * (total // parts)), BF16),
            pltpu.SemaphoreType.DMA((12,)),
            pltpu.VMEM((tall, 2 * half), F32),
            pltpu.VMEM((rows, 2 * half), F32),
            pltpu.VMEM((max(low - 1, 1), rows, 2 * half), F32),
            pltpu.VMEM((rows, 2 * half), F32),
            pltpu.VMEM((max(high - 1, 1), rows, 2 * half), F32),
            pltpu.VMEM((base, lanes), BF16),
            pltpu.VMEM((2, 2 * half, 2 * lanes), BF16),
            pltpu.VMEM((epochs, sources, lanes), F32),
            pltpu.VMEM((sources, epochs, width, lanes), F32),
            pltpu.VMEM((sources, epochs, width, lanes), F32),
            pltpu.VMEM((dirs, width, lanes), F32),
            pltpu.VMEM((dirs, width, lanes), F32),
            pltpu.VMEM((groups, width, slab), BF16),
            pltpu.VMEM((count, width, slab), BF16),
            pltpu.SemaphoreType.DMA((max(low - 1, 1),)),
            pltpu.SemaphoreType.DMA((max(low - 1, 1),)),
            pltpu.SemaphoreType.DMA((max(high - 1, 1),)),
            pltpu.SemaphoreType.DMA((max(high - 1, 1),)),
            pltpu.SemaphoreType.DMA,
            pltpu.SemaphoreType.DMA,
        ],
        compiler_params=pltpu.CompilerParams(
            collective_id=0, has_side_effects=True, vmem_limit_bytes=60 * 1024 * 1024
        ),
    )(
        cluster_of_source.reshape(sources), visibilities, baseline_coords, source_offsets, source_flux.T,
        baseline_stations.T, station_flags.T, turned(local_gains), turned(dual_gains), penalty.reshape(1, dirs),
        taper, table,
    )
    dual = dual.reshape(2, dirs, width, stations).transpose(0, 2, 1, 3)[:, None]
    return (cross, dual)


def solution(mesh):
    in_specs = (
        P(None, "tm", "chan", None),
        P(None, "tm", None),
        P(),
        P(None, "chan"),
        P(),
        P(),
        P(None, "tm"),
        P(None, "tm", "chan", None, None),
        P(None, "tm", "chan", None, None),
        P(),
    )
    out_specs = (P("chan", "tm"), P(None, "tm", "chan", None, None))
    return jax.shard_map(shards, mesh=mesh, in_specs=in_specs, out_specs=out_specs, check_vma=False)
```

```python
import math

import jax
import jax.numpy as jnp
import numpy as np
from jax import lax
from jax.experimental import pallas as pl
from jax.experimental.pallas import tpu as pltpu
from jax.sharding import PartitionSpec as P

HIGHEST = lax.Precision.HIGHEST
MESH = pl.DeviceIdType.MESH
TERMS = 3
F32 = jnp.float32
BF16 = jnp.bfloat16


def turn_polynomials():
    nodes = np.cos(np.pi * (np.arange(400) + 0.5) / 400) * 0.125 + 0.125
    root = np.sqrt(nodes)
    cosine = np.polynomial.Chebyshev.fit(nodes, np.cos(2 * np.pi * root), 6)
    sine = np.polynomial.Chebyshev.fit(nodes, np.sin(2 * np.pi * root) / root, 6)
    pick = lambda fit: [float(c) for c in fit.convert(kind=np.polynomial.Polynomial).coef]
    return pick(cosine), pick(sine)


COS_TERMS, SIN_TERMS = turn_polynomials()


def horner(terms, z):
    value = jnp.full_like(z, terms[-1])
    for term in terms[-2::-1]:
        value = value * z + term
    return value


def taper_values(total):
    angles = 2.0 * np.pi / (total - 1) * np.arange(total)
    return 0.35875 - 0.48829 * np.cos(angles) + 0.14128 * np.cos(2 * angles) - 0.01168 * np.cos(3 * angles)


def delay_tables(total, parts):
    index = np.arange(total)
    angles = 2.0 * np.pi / total * (index[:, None] * index[None, :] % total)
    wide = total // parts
    cosine = np.cos(angles).reshape(total, parts, wide)
    sine = np.sin(angles).reshape(total, parts, wide)
    return jnp.asarray(np.concatenate([cosine, sine], axis=2).transpose(1, 0, 2), BF16)


def gram_inverse(total):
    x = (2.0 * np.arange(total) + 1.0) / total - 1.0
    basis = np.stack([np.ones_like(x), x, 1.5 * x * x - 0.5], axis=1)
    return np.linalg.inv(basis.T @ basis)


def ceil_to(value, step):
    return -(-value // step) * step


def split_groups(groups):
    low = 1
    while low * 2 * low * 2 <= groups and groups % (low * 2) == 0:
        low *= 2
    return low, groups // low


def iota(shape, dim):
    return lax.broadcasted_iota(jnp.int32, shape, dim)


def make_kernel(cfg):
    groups, parts, width, dirs, stations = (cfg[k] for k in ("groups", "parts", "width", "dirs", "stations"))
    sources, epochs, base, own, pad = (cfg[k] for k in ("sources", "epochs", "base", "own", "pad"))
    low, high, rows, total = (cfg[k] for k in ("low", "high", "rows", "total"))
    count = groups * parts
    lanes = groups * pad
    half = cfg["half"]
    inverse = gram_inverse(total)
    norm2 = 1.0 / float(np.sum(taper_values(total) ** 2))
    pair_total = (epochs // 2) * parts
    slab = 2 * epochs * pad
    per_tile = 128 // pad

    def kernel(
        cluster_hbm, vis_hbm, coords_hbm, offsets_hbm, flux_hbm, pairs_hbm, flags_hbm, local_hbm, dual_hbm,
        penalty_hbm, taper_hbm, table_hbm,
        cross_out, dual_out,
        cluster, vis, coords, offsets, flux, pairs, flags, local, dual, penalty, window_buf, table_buf, load_sem,
        packed, sum_send, sum_recv, part_send, part_recv, perm, onehot, delay, wave_c, wave_s,
        pair_r, pair_i, out_send, out_recv,
        s1_send, s1_recv, s2_send, s2_recv, a_send, a_recv,
    ):
        chan = lax.axis_index("chan")
        part = lax.axis_index("tm")
        me = part * groups + chan
        barrier = pltpu.get_barrier_semaphore()

        def others(act):
            for dm in range(parts):
                m = lax.rem(part + dm, parts)

                def step(i, carry, m=m):
                    act(lax.rem(chan + i, groups), m)
                    return carry

                first = 1 if dm == 0 else 0
                lax.fori_loop(first, groups, step, 0, unroll=groups <= 16)

        lo, hi = lax.rem(chan, low), chan // low

        def greet(c, m):
            pl.semaphore_signal(barrier, inc=1, device_id={"chan": c, "tm": m}, device_id_type=MESH)

        for i in range(1, high):
            greet(lax.rem(hi + i, high) * low + lo, part)
        for i in range(1, low):
            greet(hi * low + lax.rem(lo + i, low), part)
        for i in range(1, parts):
            greet(chan, lax.rem(part + i, parts))
        loads = [
            pltpu.make_async_copy(src, dst, load_sem.at[i])
            for i, (src, dst) in enumerate(
                [
                    (penalty_hbm, penalty), (dual_hbm, dual), (local_hbm, local), (pairs_hbm, pairs),
                    (coords_hbm, coords), (offsets_hbm, offsets), (flux_hbm, flux), (flags_hbm, flags),
                    (vis_hbm, vis), (taper_hbm.at[chan], window_buf), (table_hbm.at[part], table_buf),
                    (cluster_hbm, cluster),
                ]
            )
        ]
        for load in loads:
            load.start()

        tall = dirs * width

        def coordinate(f):
            return (2 * (chan * width + f) + 1).astype(F32) / total - 1.0

        def term_of(row):
            k = sum((row >= dirs * i).astype(jnp.int32) for i in range(1, TERMS + 1))
            return k, row - k * dirs

        row, col = iota((rows, tall), 0), iota((rows, tall), 1)
        k, d = term_of(row)
        x = coordinate(lax.rem(col, width))
        value = jnp.where(k == 0, 1.0, jnp.where(k == 1, x, 1.5 * x * x - 0.5))
        weights = jnp.where((d == col // width) & (k < TERMS), value, 0.0)
        prow, pcol = iota((base, lanes), 0), iota((base, lanes), 1)
        inner = lax.rem(pcol, pad)
        perm[...] = jnp.where((prow == (pcol // pad) * own + inner) & (inner < own), 1.0, 0.0).astype(BF16)
        packed[...] = jnp.zeros_like(packed)
        for load in loads[:3]:
            load.wait()
        rate = jnp.sum(
            jnp.where(iota((tall, dirs), 0) // width == iota((tall, dirs), 1), penalty[...], 0.0), axis=1, keepdims=True
        )
        inverse_rate = 1.0 / rate
        for r in range(2):
            packed[:, r * half : r * half + stations] = local[r] + dual[r] * inverse_rate

        acc = jnp.dot(weights, packed[...], precision=HIGHEST, preferred_element_type=F32)
        sum_send[...] = acc
        pl.semaphore_wait(barrier, low + high + parts - 3)

        def stage(src, dst, send, recv, size, mine, address):
            copies = []
            for i in range(1, size):
                copies.append(
                    pltpu.make_async_remote_copy(
                        src_ref=src,
                        dst_ref=dst.at[i - 1],
                        send_sem=send.at[i - 1],
                        recv_sem=recv.at[i - 1],
                        device_id={"chan": address(lax.rem(mine + i, size)), "tm": part},
                        device_id_type=MESH,
                    )
                )
            for copy in copies:
                copy.start()
            return copies

        first = stage(sum_send, sum_recv, s1_send, s1_recv, low, lo, lambda t: hi * low + t)
        for load in loads[3:]:
            load.wait()
        place = perm[...]
        station_rows = jnp.dot(pairs[...].astype(F32).astype(BF16), place, preferred_element_type=F32).astype(jnp.int32)
        srow = iota((2 * half, lanes), 0)
        for side in range(2):
            line = station_rows[side : side + 1, :]
            for r in range(2):
                onehot[r, :, side * lanes : (side + 1) * lanes] = jnp.where(srow == line + r * half, 1.0, 0.0).astype(BF16)

        def placed(value):
            out = None
            for _ in range(3):
                piece = value.astype(BF16)
                value = value - piece.astype(F32)
                moved = jnp.dot(piece, place, preferred_element_type=F32)
                out = moved if out is None else out + moved
            return out

        u, v, w = (placed(coords[i]) for i in range(3))
        same = iota((sources, sources), 0) == iota((sources, sources), 1)
        column = lambda line: jnp.sum(jnp.where(same, line, 0.0), axis=1, keepdims=True)
        l, m = offsets[0:1, :], offsets[1:2, :]
        lc, mc, nc = column(l), column(m), column(jnp.sqrt(1.0 - l * l - m * m) - 1.0)
        for t in range(epochs):
            delay[t] = lc * u[t : t + 1] + mc * v[t : t + 1] + nc * w[t : t + 1]
        vis_placed = [
            [jnp.dot(vis[r, t].astype(F32).astype(BF16), place, preferred_element_type=F32) for t in range(epochs)]
            for r in range(2)
        ]
        unflagged = (1.0 - flags[...].astype(F32)).astype(BF16)
        kept = jnp.dot(unflagged, onehot[0, 0:stations, :], preferred_element_type=F32)
        keep = kept[:, :lanes] * kept[:, lanes:]
        channel = (chan * width + iota((width, 1), 0)).astype(F32)
        rate_turns = 0.9 + 0.2 * (channel + 0.5) / total

        def phases(begin, end):
            for s in range(begin, end):
                scale = flux[:, s : s + 1]
                for t in range(epochs):
                    turns = rate_turns * delay[t, s : s + 1, :]
                    turns = turns - jnp.round(turns)
                    z = turns * turns
                    wave_c[s, t] = scale * horner(COS_TERMS, z)
                    wave_s[s, t] = scale * (turns * horner(SIN_TERMS, z))

        phases(0, sources // 2)
        for i, copy in enumerate(first):
            copy.wait_recv()
            acc = acc + sum_recv[i]
        part_send[...] = acc
        second = stage(part_send, part_recv, s2_send, s2_recv, high, hi, lambda t: t * low + lo)
        phases(sources // 2, sources)
        vrow, vcol = iota((tall, rows), 0), iota((tall, rows), 1)
        k, d = term_of(vcol)
        x = coordinate(lax.rem(vrow, width))
        x2 = 1.5 * x * x - 0.5
        value = jnp.zeros_like(x)
        for i in range(TERMS):
            mixed = float(inverse[0, i]) + x * float(inverse[1, i]) + x2 * float(inverse[2, i])
            value = jnp.where(k == i, mixed, value)
        spread = jnp.where((d == vrow // width) & (k < TERMS), value, 0.0)
        for i, copy in enumerate(second):
            copy.wait_recv()
            acc = acc + part_recv[i]

        smooth = jnp.dot(spread, acc, precision=HIGHEST, preferred_element_type=F32)
        big = smooth.astype(BF16)
        small = (smooth - big.astype(F32)).astype(BF16)
        gains = [
            jnp.dot(big, onehot[r], preferred_element_type=F32) + jnp.dot(small, onehot[r], preferred_element_type=F32)
            for r in range(2)
        ]
        for d in range(dirs):
            band = slice(d * width, (d + 1) * width)
            pr, pi = gains[0][band, :lanes], gains[1][band, :lanes]
            qr, qi = gains[0][band, lanes:], gains[1][band, lanes:]
            pair_r[d] = pr * qr + pi * qi
            pair_i[d] = pi * qr - pr * qi
        model_r = [jnp.zeros((width, lanes), F32) for _ in range(epochs)]
        model_i = [jnp.zeros((width, lanes), F32) for _ in range(epochs)]
        for s in range(sources):
            which = cluster[s]
            gr, gi = pair_r[which], pair_i[which]
            for t in range(epochs):
                c, n = wave_c[s, t], wave_s[s, t]
                model_r[t] = model_r[t] + (gr * c + gi * n)
                model_i[t] = model_i[t] + (gi * c - gr * n)
        window = window_buf[...]
        tiles = []
        for r in range(2):
            for t in range(epochs):
                left = vis_placed[r][t] - (model_r[t] if r == 0 else model_i[t])
                left = (keep[t : t + 1, :] * left).astype(BF16).astype(F32)
                tiles.append((left * window[:, 0:1]).astype(BF16).astype(F32))
        slot = iota((width, 128), 1) // pad
        for c in range(groups):
            tile, place_in = c // per_tile, c % per_tile
            for start in range(0, len(tiles), per_tile):
                block = None
                for j in range(per_tile):
                    piece = tiles[start + j][:, tile * 128 : (tile + 1) * 128]
                    shift = ((j - place_in) * pad) % 128
                    piece = pltpu.roll(piece, shift, 1) if shift else piece
                    block = piece if block is None else jnp.where(slot == j, piece, block)
                out_send[c, :, start * pad : start * pad + 128] = block.astype(BF16)
        out_recv[me] = out_send[chan]

        def push(c, m):
            return pltpu.make_async_remote_copy(
                src_ref=out_send.at[c],
                dst_ref=out_recv.at[me],
                send_sem=a_send,
                recv_sem=a_recv,
                device_id={"chan": c, "tm": m},
                device_id_type=MESH,
            )

        others(lambda c, m: push(c, m).start())

        for r in range(2):
            dual_out[r] = dual[r] + rate * (local[r] - smooth[:, r * half : r * half + stations])
        for copy in first + second:
            copy.wait_send()

        whole = pltpu.make_async_remote_copy(
            src_ref=out_recv.at[pl.ds(0, count - 1)],
            dst_ref=out_recv.at[pl.ds(0, count - 1)],
            send_sem=a_send,
            recv_sem=a_recv,
            device_id={"chan": lax.rem(chan + 1, groups), "tm": part},
            device_id_type=MESH,
        )
        whole.wait_recv()
        wide = total // parts
        kernel_table = table_buf[...]
        cross = jnp.zeros((pad, wide), F32)
        for m in range(parts):
            grid = out_recv[m * groups : (m + 1) * groups].astype(F32).reshape(total, slab)
            raw = jnp.dot(grid.T.astype(BF16), kernel_table, preferred_element_type=F32)
            rest = epochs * pad
            real = raw[:rest, :wide] + raw[rest:, wide:]
            imag = raw[rest:, :wide] - raw[:rest, wide:]
            for j in range(epochs // 2):
                a, b = slice(2 * j * pad, (2 * j + 1) * pad), slice((2 * j + 1) * pad, (2 * j + 2) * pad)
                cross = cross + (real[a] * real[b] + imag[a] * imag[b])
        cross_out[...] = cross[:own] * (norm2 / pair_total)
        whole.wait_send()

    return kernel


def hand_over(cross_in, dual_in, cross_out, dual_out):
    cross_out[...] = cross_in[...]
    dual_out[...] = dual_in[...]


def shards(
    visibilities, baseline_coords, source_offsets, source_flux, cluster_of_source,
    baseline_stations, station_flags, local_gains, dual_gains, penalty,
):
    groups, parts = lax.axis_size("chan"), lax.axis_size("tm")
    sources, width = source_flux.shape
    _, epochs, _, base = visibilities.shape
    _, _, _, dirs, stations = local_gains.shape
    total = width * groups
    own = base // groups
    pad = ceil_to(own, 32)
    lanes = groups * pad
    half = ceil_to(stations, 64)
    rows = ceil_to(TERMS * dirs, 8)
    low, high = split_groups(groups)
    tall = dirs * width
    slab = 2 * epochs * pad
    count = groups * parts
    cfg = dict(
        groups=groups, parts=parts, width=width, dirs=dirs, stations=stations, sources=sources, epochs=epochs,
        base=base, own=own, pad=pad, low=low, high=high, rows=rows, total=total, half=half,
    )
    taper = jnp.asarray(np.broadcast_to(taper_values(total).reshape(groups, width, 1), (groups, width, 128)), F32)
    table = delay_tables(total, parts)
    turned = lambda a: a[:, 0].transpose(0, 2, 1, 3).reshape(2, tall, stations)
    vmem = pl.BlockSpec(memory_space=pltpu.VMEM)
    cross, dual = pl.pallas_call(
        make_kernel(cfg),
        out_shape=(
            jax.ShapeDtypeStruct((own, total // parts), F32),
            jax.ShapeDtypeStruct((2, tall, stations), F32),
        ),
        in_specs=[pl.BlockSpec(memory_space=pltpu.HBM)] * 12,
        out_specs=(vmem, vmem),
        scratch_shapes=[
            pltpu.SMEM((sources,), jnp.int32),
            pltpu.VMEM(visibilities.shape, BF16),
            pltpu.VMEM(baseline_coords.shape, F32),
            pltpu.VMEM(source_offsets.shape, F32),
            pltpu.VMEM((width, sources), F32),
            pltpu.VMEM((2, base), jnp.int32),
            pltpu.VMEM((epochs, stations), jnp.int32),
            pltpu.VMEM((2, tall, stations), F32),
            pltpu.VMEM((2, tall, stations), F32),
            pltpu.VMEM((1, dirs), F32),
            pltpu.VMEM((width, 128), F32),
            pltpu.VMEM((total, 2 * (total // parts)), BF16),
            pltpu.SemaphoreType.DMA((12,)),
            pltpu.VMEM((tall, 2 * half), F32),
            pltpu.VMEM((rows, 2 * half), F32),
            pltpu.VMEM((max(low - 1, 1), rows, 2 * half), F32),
            pltpu.VMEM((rows, 2 * half), F32),
            pltpu.VMEM((max(high - 1, 1), rows, 2 * half), F32),
            pltpu.VMEM((base, lanes), BF16),
            pltpu.VMEM((2, 2 * half, 2 * lanes), BF16),
            pltpu.VMEM((epochs, sources, lanes), F32),
            pltpu.VMEM((sources, epochs, width, lanes), F32),
            pltpu.VMEM((sources, epochs, width, lanes), F32),
            pltpu.VMEM((dirs, width, lanes), F32),
            pltpu.VMEM((dirs, width, lanes), F32),
            pltpu.VMEM((groups, width, slab), BF16),
            pltpu.VMEM((count, width, slab), BF16),
            pltpu.SemaphoreType.DMA((max(low - 1, 1),)),
            pltpu.SemaphoreType.DMA((max(low - 1, 1),)),
            pltpu.SemaphoreType.DMA((max(high - 1, 1),)),
            pltpu.SemaphoreType.DMA((max(high - 1, 1),)),
            pltpu.SemaphoreType.DMA,
            pltpu.SemaphoreType.DMA,
        ],
        compiler_params=pltpu.CompilerParams(
            collective_id=0, has_side_effects=True, vmem_limit_bytes=60 * 1024 * 1024
        ),
    )(
        cluster_of_source.reshape(sources), visibilities, baseline_coords, source_offsets, source_flux.T,
        baseline_stations.T, station_flags.T, turned(local_gains), turned(dual_gains), penalty.reshape(1, dirs),
        taper, table,
    )
    cross, dual = pl.pallas_call(
        hand_over,
        out_shape=(
            jax.ShapeDtypeStruct(cross.shape, F32),
            jax.ShapeDtypeStruct(dual.shape, F32),
        ),
        in_specs=[vmem, vmem],
        out_specs=(vmem, vmem),
    )(cross, dual)
    dual = dual.reshape(2, dirs, width, stations).transpose(0, 2, 1, 3)[:, None]
    return (cross, dual)


def solution(mesh):
    in_specs = (
        P(None, "tm", "chan", None),
        P(None, "tm", None),
        P(),
        P(None, "chan"),
        P(),
        P(),
        P(None, "tm"),
        P(None, "tm", "chan", None, None),
        P(None, "tm", "chan", None, None),
        P(),
    )
    out_specs = (P("chan", "tm"), P(None, "tm", "chan", None, None))
    return jax.shard_map(shards, mesh=mesh, in_specs=in_specs, out_specs=out_specs, check_vma=False)
```

```python
import math

import jax
import jax.numpy as jnp
import numpy as np
from jax import lax
from jax.experimental import pallas as pl
from jax.experimental.pallas import tpu as pltpu
from jax.sharding import PartitionSpec as P

HIGHEST = lax.Precision.HIGHEST
MESH = pl.DeviceIdType.MESH
TERMS = 3
F32 = jnp.float32
BF16 = jnp.bfloat16


def turn_polynomials():
    nodes = np.cos(np.pi * (np.arange(400) + 0.5) / 400) * 0.125 + 0.125
    root = np.sqrt(nodes)
    cosine = np.polynomial.Chebyshev.fit(nodes, np.cos(2 * np.pi * root), 6)
    sine = np.polynomial.Chebyshev.fit(nodes, np.sin(2 * np.pi * root) / root, 6)
    pick = lambda fit: [float(c) for c in fit.convert(kind=np.polynomial.Polynomial).coef]
    return pick(cosine), pick(sine)


COS_TERMS, SIN_TERMS = turn_polynomials()


def horner(terms, z):
    value = jnp.full_like(z, terms[-1])
    for term in terms[-2::-1]:
        value = value * z + term
    return value


def taper_values(total):
    angles = 2.0 * np.pi / (total - 1) * np.arange(total)
    return 0.35875 - 0.48829 * np.cos(angles) + 0.14128 * np.cos(2 * angles) - 0.01168 * np.cos(3 * angles)


def delay_tables(total, parts):
    index = np.arange(total)
    angles = 2.0 * np.pi / total * (index[:, None] * index[None, :] % total)
    wide = total // parts
    cosine = np.cos(angles).reshape(total, parts, wide)
    sine = np.sin(angles).reshape(total, parts, wide)
    return jnp.asarray(np.concatenate([cosine, sine], axis=2).transpose(1, 0, 2), BF16)


def gram_inverse(total):
    x = (2.0 * np.arange(total) + 1.0) / total - 1.0
    basis = np.stack([np.ones_like(x), x, 1.5 * x * x - 0.5], axis=1)
    return np.linalg.inv(basis.T @ basis)


def ceil_to(value, step):
    return -(-value // step) * step


def split_groups(groups):
    low = 1
    while low * 2 * low * 2 <= groups and groups % (low * 2) == 0:
        low *= 2
    return low, groups // low


def iota(shape, dim):
    return lax.broadcasted_iota(jnp.int32, shape, dim)


def make_kernel(cfg):
    groups, parts, width, dirs, stations = (cfg[k] for k in ("groups", "parts", "width", "dirs", "stations"))
    sources, epochs, base, own, pad = (cfg[k] for k in ("sources", "epochs", "base", "own", "pad"))
    low, high, rows, total = (cfg[k] for k in ("low", "high", "rows", "total"))
    count = groups * parts
    lanes = groups * pad
    half = cfg["half"]
    inverse = gram_inverse(total)
    norm2 = 1.0 / float(np.sum(taper_values(total) ** 2))
    pair_total = (epochs // 2) * parts
    slab = 2 * epochs * pad
    per_tile = 128 // pad

    def kernel(
        cluster_hbm, vis_hbm, coords_hbm, offsets_hbm, flux_hbm, pairs_hbm, flags_hbm, local_hbm, dual_hbm,
        penalty_hbm, taper_hbm, table_hbm,
        cross_out, dual_out,
        cluster, vis, coords, offsets, flux, pairs, flags, local, dual, penalty, window_buf, table_buf, load_sem,
        packed, sum_send, sum_recv, part_send, part_recv, perm, onehot, delay, wave_c, wave_s,
        pair_r, pair_i, out_send, out_recv,
        s1_send, s1_recv, s2_send, s2_recv, a_send, a_recv,
    ):
        chan = lax.axis_index("chan")
        part = lax.axis_index("tm")
        me = part * groups + chan
        barrier = pltpu.get_barrier_semaphore()

        def others(act):
            for dm in range(parts):
                m = lax.rem(part + dm, parts)

                def step(i, carry, m=m):
                    act(lax.rem(chan + i, groups), m)
                    return carry

                first = 1 if dm == 0 else 0
                lax.fori_loop(first, groups, step, 0, unroll=groups <= 16)

        lo, hi = lax.rem(chan, low), chan // low

        def greet(c, m):
            pl.semaphore_signal(barrier, inc=1, device_id={"chan": c, "tm": m}, device_id_type=MESH)

        for i in range(1, high):
            greet(lax.rem(hi + i, high) * low + lo, part)
        for i in range(1, low):
            greet(hi * low + lax.rem(lo + i, low), part)
        for i in range(1, parts):
            greet(chan, lax.rem(part + i, parts))
        loads = [
            pltpu.make_async_copy(src, dst, load_sem.at[i])
            for i, (src, dst) in enumerate(
                [
                    (penalty_hbm, penalty), (dual_hbm, dual), (local_hbm, local), (pairs_hbm, pairs),
                    (coords_hbm, coords), (offsets_hbm, offsets), (flux_hbm, flux), (flags_hbm, flags),
                    (vis_hbm, vis), (taper_hbm.at[chan], window_buf), (table_hbm.at[part], table_buf),
                    (cluster_hbm, cluster),
                ]
            )
        ]
        for load in loads:
            load.start()

        tall = dirs * width

        def coordinate(f):
            return (2 * (chan * width + f) + 1).astype(F32) / total - 1.0

        def term_of(row):
            k = sum((row >= dirs * i).astype(jnp.int32) for i in range(1, TERMS + 1))
            return k, row - k * dirs

        row, col = iota((rows, tall), 0), iota((rows, tall), 1)
        k, d = term_of(row)
        x = coordinate(lax.rem(col, width))
        value = jnp.where(k == 0, 1.0, jnp.where(k == 1, x, 1.5 * x * x - 0.5))
        weights = jnp.where((d == col // width) & (k < TERMS), value, 0.0)
        prow, pcol = iota((base, lanes), 0), iota((base, lanes), 1)
        inner = lax.rem(pcol, pad)
        perm[...] = jnp.where((prow == (pcol // pad) * own + inner) & (inner < own), 1.0, 0.0).astype(BF16)
        packed[...] = jnp.zeros_like(packed)
        for load in loads[:3]:
            load.wait()
        rate = jnp.sum(
            jnp.where(iota((tall, dirs), 0) // width == iota((tall, dirs), 1), penalty[...], 0.0), axis=1, keepdims=True
        )
        inverse_rate = 1.0 / rate
        for r in range(2):
            packed[:, r * half : r * half + stations] = local[r] + dual[r] * inverse_rate

        acc = jnp.dot(weights, packed[...], precision=HIGHEST, preferred_element_type=F32)
        sum_send[...] = acc
        pl.semaphore_wait(barrier, low + high + parts - 3)

        def stage(src, dst, send, recv, size, mine, address):
            copies = []
            for i in range(1, size):
                copies.append(
                    pltpu.make_async_remote_copy(
                        src_ref=src,
                        dst_ref=dst.at[i - 1],
                        send_sem=send.at[i - 1],
                        recv_sem=recv.at[i - 1],
                        device_id={"chan": address(lax.rem(mine + i, size)), "tm": part},
                        device_id_type=MESH,
                    )
                )
            for copy in copies:
                copy.start()
            return copies

        first = stage(sum_send, sum_recv, s1_send, s1_recv, low, lo, lambda t: hi * low + t)
        for load in loads[3:]:
            load.wait()
        place = perm[...]
        station_rows = jnp.dot(pairs[...].astype(F32).astype(BF16), place, preferred_element_type=F32).astype(jnp.int32)
        srow = iota((2 * half, lanes), 0)
        for side in range(2):
            line = station_rows[side : side + 1, :]
            for r in range(2):
                onehot[r, :, side * lanes : (side + 1) * lanes] = jnp.where(srow == line + r * half, 1.0, 0.0).astype(BF16)

        def placed(value):
            out = None
            for _ in range(3):
                piece = value.astype(BF16)
                value = value - piece.astype(F32)
                moved = jnp.dot(piece, place, preferred_element_type=F32)
                out = moved if out is None else out + moved
            return out

        u, v, w = (placed(coords[i]) for i in range(3))
        same = iota((sources, sources), 0) == iota((sources, sources), 1)
        column = lambda line: jnp.sum(jnp.where(same, line, 0.0), axis=1, keepdims=True)
        l, m = offsets[0:1, :], offsets[1:2, :]
        lc, mc, nc = column(l), column(m), column(jnp.sqrt(1.0 - l * l - m * m) - 1.0)
        for t in range(epochs):
            delay[t] = lc * u[t : t + 1] + mc * v[t : t + 1] + nc * w[t : t + 1]
        vis_placed = [
            [jnp.dot(vis[r, t].astype(F32).astype(BF16), place, preferred_element_type=F32) for t in range(epochs)]
            for r in range(2)
        ]
        unflagged = (1.0 - flags[...].astype(F32)).astype(BF16)
        kept = jnp.dot(unflagged, onehot[0, 0:stations, :], preferred_element_type=F32)
        keep = kept[:, :lanes] * kept[:, lanes:]
        channel = (chan * width + iota((width, 1), 0)).astype(F32)
        rate_turns = 0.9 + 0.2 * (channel + 0.5) / total

        def phases(begin, end):
            for s in range(begin, end):
                scale = flux[:, s : s + 1]
                for t in range(epochs):
                    turns = rate_turns * delay[t, s : s + 1, :]
                    turns = turns - jnp.round(turns)
                    z = turns * turns
                    wave_c[s, t] = scale * horner(COS_TERMS, z)
                    wave_s[s, t] = scale * (turns * horner(SIN_TERMS, z))

        phases(0, sources // 2)
        for i, copy in enumerate(first):
            copy.wait_recv()
            acc = acc + sum_recv[i]
        part_send[...] = acc
        second = stage(part_send, part_recv, s2_send, s2_recv, high, hi, lambda t: t * low + lo)
        phases(sources // 2, sources)
        vrow, vcol = iota((tall, rows), 0), iota((tall, rows), 1)
        k, d = term_of(vcol)
        x = coordinate(lax.rem(vrow, width))
        x2 = 1.5 * x * x - 0.5
        value = jnp.zeros_like(x)
        for i in range(TERMS):
            mixed = float(inverse[0, i]) + x * float(inverse[1, i]) + x2 * float(inverse[2, i])
            value = jnp.where(k == i, mixed, value)
        spread = jnp.where((d == vrow // width) & (k < TERMS), value, 0.0)
        for i, copy in enumerate(second):
            copy.wait_recv()
            acc = acc + part_recv[i]

        smooth = jnp.dot(spread, acc, precision=HIGHEST, preferred_element_type=F32)
        big = smooth.astype(BF16)
        small = (smooth - big.astype(F32)).astype(BF16)
        gains = [
            jnp.dot(big, onehot[r], preferred_element_type=F32) + jnp.dot(small, onehot[r], preferred_element_type=F32)
            for r in range(2)
        ]
        for d in range(dirs):
            band = slice(d * width, (d + 1) * width)
            pr, pi = gains[0][band, :lanes], gains[1][band, :lanes]
            qr, qi = gains[0][band, lanes:], gains[1][band, lanes:]
            pair_r[d] = pr * qr + pi * qi
            pair_i[d] = pi * qr - pr * qi
        model_r = [jnp.zeros((width, lanes), F32) for _ in range(epochs)]
        model_i = [jnp.zeros((width, lanes), F32) for _ in range(epochs)]
        for s in range(sources):
            which = cluster[s]
            gr, gi = pair_r[which], pair_i[which]
            for t in range(epochs):
                c, n = wave_c[s, t], wave_s[s, t]
                model_r[t] = model_r[t] + (gr * c + gi * n)
                model_i[t] = model_i[t] + (gi * c - gr * n)
        window = window_buf[...]
        tiles = []
        for r in range(2):
            for t in range(epochs):
                left = vis_placed[r][t] - (model_r[t] if r == 0 else model_i[t])
                left = (keep[t : t + 1, :] * left).astype(BF16).astype(F32)
                tiles.append((left * window[:, 0:1]).astype(BF16).astype(F32))
        slot = iota((width, 128), 1) // pad
        for c in range(groups):
            tile, place_in = c // per_tile, c % per_tile
            for start in range(0, len(tiles), per_tile):
                block = None
                for j in range(per_tile):
                    piece = tiles[start + j][:, tile * 128 : (tile + 1) * 128]
                    shift = ((j - place_in) * pad) % 128
                    piece = pltpu.roll(piece, shift, 1) if shift else piece
                    block = piece if block is None else jnp.where(slot == j, piece, block)
                out_send[c, :, start * pad : start * pad + 128] = block.astype(BF16)
        out_recv[me] = out_send[chan]

        def push(c, m):
            return pltpu.make_async_remote_copy(
                src_ref=out_send.at[c],
                dst_ref=out_recv.at[me],
                send_sem=a_send,
                recv_sem=a_recv,
                device_id={"chan": c, "tm": m},
                device_id_type=MESH,
            )

        others(lambda c, m: push(c, m).start())

        for r in range(2):
            dual_out[r] = dual[r] + rate * (local[r] - smooth[:, r * half : r * half + stations])
        for copy in first + second:
            copy.wait_send()

        whole = pltpu.make_async_remote_copy(
            src_ref=out_recv.at[pl.ds(0, count - 1)],
            dst_ref=out_recv.at[pl.ds(0, count - 1)],
            send_sem=a_send,
            recv_sem=a_recv,
            device_id={"chan": lax.rem(chan + 1, groups), "tm": part},
            device_id_type=MESH,
        )
        whole.wait_recv()
        wide = total // parts
        kernel_table = table_buf[...]
        cross = jnp.zeros((pad, wide), F32)
        for m in range(parts):
            grid = out_recv[m * groups : (m + 1) * groups].astype(F32).reshape(total, slab)
            raw = jnp.dot(grid.T.astype(BF16), kernel_table, preferred_element_type=F32)
            rest = epochs * pad
            real = raw[:rest, :wide] + raw[rest:, wide:]
            imag = raw[rest:, :wide] - raw[:rest, wide:]
            for j in range(epochs // 2):
                a, b = slice(2 * j * pad, (2 * j + 1) * pad), slice((2 * j + 1) * pad, (2 * j + 2) * pad)
                cross = cross + (real[a] * real[b] + imag[a] * imag[b])
        cross_out[...] = cross[:own] * (norm2 / pair_total)
        whole.wait_send()

    return kernel


def hand_over(cross_in, dual_in, cross_out, dual_out):
    cross_out[...] = cross_in[...]
    dual_out[...] = dual_in[...]


def shards(
    visibilities, baseline_coords, source_offsets, source_flux, cluster_of_source,
    baseline_stations, station_flags, local_gains, dual_gains, penalty,
):
    groups, parts = lax.axis_size("chan"), lax.axis_size("tm")
    sources, width = source_flux.shape
    _, epochs, _, base = visibilities.shape
    _, _, _, dirs, stations = local_gains.shape
    total = width * groups
    own = base // groups
    pad = ceil_to(own, 32)
    lanes = groups * pad
    half = ceil_to(stations, 64)
    rows = ceil_to(TERMS * dirs, 8)
    low, high = split_groups(groups)
    tall = dirs * width
    slab = 2 * epochs * pad
    count = groups * parts
    cfg = dict(
        groups=groups, parts=parts, width=width, dirs=dirs, stations=stations, sources=sources, epochs=epochs,
        base=base, own=own, pad=pad, low=low, high=high, rows=rows, total=total, half=half,
    )
    taper = jnp.asarray(np.broadcast_to(taper_values(total).reshape(groups, width, 1), (groups, width, 128)), F32)
    table = delay_tables(total, parts)
    turned = lambda a: a[:, 0].transpose(0, 2, 1, 3).reshape(2, tall, stations)
    vmem = pl.BlockSpec(memory_space=pltpu.VMEM)
    cross, dual = pl.pallas_call(
        make_kernel(cfg),
        out_shape=(
            jax.ShapeDtypeStruct((own, total // parts), F32),
            jax.ShapeDtypeStruct((2, tall, stations), F32),
        ),
        in_specs=[pl.BlockSpec(memory_space=pltpu.HBM)] * 12,
        out_specs=(vmem, vmem),
        scratch_shapes=[
            pltpu.SMEM((sources,), jnp.int32),
            pltpu.VMEM(visibilities.shape, BF16),
            pltpu.VMEM(baseline_coords.shape, F32),
            pltpu.VMEM(source_offsets.shape, F32),
            pltpu.VMEM((width, sources), F32),
            pltpu.VMEM((2, base), jnp.int32),
            pltpu.VMEM((epochs, stations), jnp.int32),
            pltpu.VMEM((2, tall, stations), F32),
            pltpu.VMEM((2, tall, stations), F32),
            pltpu.VMEM((1, dirs), F32),
            pltpu.VMEM((width, 128), F32),
            pltpu.VMEM((total, 2 * (total // parts)), BF16),
            pltpu.SemaphoreType.DMA((12,)),
            pltpu.VMEM((tall, 2 * half), F32),
            pltpu.VMEM((rows, 2 * half), F32),
            pltpu.VMEM((max(low - 1, 1), rows, 2 * half), F32),
            pltpu.VMEM((rows, 2 * half), F32),
            pltpu.VMEM((max(high - 1, 1), rows, 2 * half), F32),
            pltpu.VMEM((base, lanes), BF16),
            pltpu.VMEM((2, 2 * half, 2 * lanes), BF16),
            pltpu.VMEM((epochs, sources, lanes), F32),
            pltpu.VMEM((sources, epochs, width, lanes), F32),
            pltpu.VMEM((sources, epochs, width, lanes), F32),
            pltpu.VMEM((dirs, width, lanes), F32),
            pltpu.VMEM((dirs, width, lanes), F32),
            pltpu.VMEM((groups, width, slab), BF16),
            pltpu.VMEM((count, width, slab), BF16),
            pltpu.SemaphoreType.DMA((max(low - 1, 1),)),
            pltpu.SemaphoreType.DMA((max(low - 1, 1),)),
            pltpu.SemaphoreType.DMA((max(high - 1, 1),)),
            pltpu.SemaphoreType.DMA((max(high - 1, 1),)),
            pltpu.SemaphoreType.DMA,
            pltpu.SemaphoreType.DMA,
        ],
        compiler_params=pltpu.CompilerParams(
            collective_id=0, has_side_effects=True, vmem_limit_bytes=40 * 1024 * 1024
        ),
    )(
        cluster_of_source.reshape(sources), visibilities, baseline_coords, source_offsets, source_flux.T,
        baseline_stations.T, station_flags.T, turned(local_gains), turned(dual_gains), penalty.reshape(1, dirs),
        taper, table,
    )
    cross, dual = pl.pallas_call(
        hand_over,
        out_shape=(
            jax.ShapeDtypeStruct(cross.shape, F32),
            jax.ShapeDtypeStruct(dual.shape, F32),
        ),
        in_specs=[vmem, vmem],
        out_specs=(vmem, vmem),
    )(cross, dual)
    dual = dual.reshape(2, dirs, width, stations).transpose(0, 2, 1, 3)[:, None]
    return (cross, dual)


def solution(mesh):
    in_specs = (
        P(None, "tm", "chan", None),
        P(None, "tm", None),
        P(),
        P(None, "chan"),
        P(),
        P(),
        P(None, "tm"),
        P(None, "tm", "chan", None, None),
        P(None, "tm", "chan", None, None),
        P(),
    )
    out_specs = (P("chan", "tm"), P(None, "tm", "chan", None, None))
    return jax.shard_map(shards, mesh=mesh, in_specs=in_specs, out_specs=out_specs, check_vma=False)
```
